128 devices in a mesh: seq: 4 (over x), head: 32 (over y, z, core).
Axes of the slice: x: 4, y: 4, z: 4, core: 2. Of those that a mesh axis runs over, the one named last changes fastest.
Arguments:
- queries: bfloat16 [32768, 4096], P(('seq', 'head')), may hold values from -6 to 6
- key_vectors: bfloat16 [32768, 4096], P(('seq', 'head')), may hold values from -0.375 to 0.375
- values: bfloat16 [32768, 8192], P(('seq', 'head')), may hold values from -6 to 6
- decay_log: bfloat16 [32768, 16], P(('seq', 'head')), may hold values from -0.8 to 0, as said below
- gate_input: bfloat16 [32768, 8192], P(('seq', 'head')), may hold values from -6 to 6
Outputs:
- retention_out: bfloat16 [32768, 8192], P(('seq', 'head'))
The draws below stay inside these ranges and needn't reach their ends.
Inputs may be any that keep to these rules, and one draw needn't show every extreme that they name: `decay_log`: every entry is negative.
All inputs are finite; a program needn't handle non-finite values.
Results may differ from the reference program's by a relative error of at most 0.0063.
Values may be sent and summed in bfloat16 or wider, within the bound.
A program may use at most 128 MiB of HBM per device.

```python
import math
import jax
import jax.numpy as jnp
from jax import lax

RETAIN_HEADS = 16
DK = 256
DV = 512
BLOCK = 512
DOC_POSITIONS = 32768


def draw_decay_log(key, part):
    key_kind, key_slow, key_fast, key_rough, key_location, key_magnitude, key_medium = jax.random.split(key, 7)
    fast_count = 4
    medium_count = 4
    medium_low = math.log(1.0 / 600.0)
    medium_high = math.log(1.0 / 300.0)
    head_rank = jax.random.permutation(key_kind, jnp.arange(RETAIN_HEADS, dtype=jnp.int32))
    fast_heads = head_rank < fast_count
    medium_heads = jnp.logical_and(head_rank >= fast_count, head_rank < fast_count + medium_count)
    slow_rate = jnp.exp(jax.random.uniform(key_slow, (RETAIN_HEADS,), jnp.float32, math.log(0.2), math.log(0.5))) / DOC_POSITIONS
    fast_rate = jnp.exp(jax.random.uniform(key_fast, (RETAIN_HEADS,), jnp.float32, math.log(1.0 / 50.0), math.log(1.0 / 30.0)))
    medium_rate = jnp.exp(jax.random.uniform(key_medium, (RETAIN_HEADS,), jnp.float32, medium_low, medium_high))
    head_decay_rate = jnp.where(fast_heads, fast_rate, jnp.where(medium_heads, medium_rate, slow_rate))
    jaggedness = jnp.exp(jax.random.uniform(key_rough, (DOC_POSITIONS, RETAIN_HEADS), jnp.float32, math.log(0.5), math.log(2.0)))
    key_first, key_gap = jax.random.split(key_location)
    first_spot = jax.random.randint(key_first, (RETAIN_HEADS,), 0, DOC_POSITIONS)
    spot_gap = jax.random.randint(key_gap, (RETAIN_HEADS,), 0, DOC_POSITIONS - 1)
    second_spot = (first_spot + 1 + spot_gap) % DOC_POSITIONS
    spike_magnitude = jax.random.uniform(key_magnitude, (2, RETAIN_HEADS), jnp.float32, math.log(0.5), math.log(0.8))
    token_offset = jnp.arange(DOC_POSITIONS)[:, None]
    decay_spikes = jnp.where(token_offset == first_spot[None, :], spike_magnitude[0][None, :], 0.0)
    decay_spikes = decay_spikes + jnp.where(token_offset == second_spot[None, :], spike_magnitude[1][None, :], 0.0)
    return (decay_spikes - head_decay_rate[None, :] * jaggedness).astype(jnp.bfloat16)


def block_scale(key, extent, cuts, low, high):
    level, own = 1.0, jax.random.fold_in(key, 6)
    for dim, shards_of in cuts:
        heights = jnp.exp(jax.random.uniform(jax.random.fold_in(own, dim), (shards_of,), jnp.float32, low / len(cuts), high / len(cuts)))
        level = level * jnp.repeat(heights, extent[dim] // shards_of).reshape([-1 if axis == dim else 1 for axis in range(len(extent))])
    return level


def bell_draw(own_key, shape, deviation, reach, shards=(), held_as=jnp.bfloat16):
    factor_of = block_scale(own_key, shape, shards, -0.22, 0.18) if shards else 1.0
    array = jax.random.normal(own_key, shape, jnp.float32) * deviation * factor_of
    return jnp.minimum(jnp.maximum(array, -reach), reach).astype(held_as)


def setup_inputs(seed: int = 0) -> dict:
    key_of = jax.random.split(jax.random.key(seed), 6)
    return {
        "queries": bell_draw(key_of[0], (DOC_POSITIONS, RETAIN_HEADS * DK), 1.0, 6.0, ((0, 128),)),
        "key_vectors": bell_draw(key_of[1], (DOC_POSITIONS, RETAIN_HEADS * DK), 0.0625, 0.375, ((0, 128),)),
        "values": bell_draw(key_of[2], (DOC_POSITIONS, RETAIN_HEADS * DV), 1.0, 6.0, ((0, 128),)),
        "decay_log": draw_decay_log(jax.random.fold_in(key_of[5], 71), 0),
        "gate_input": bell_draw(key_of[4], (DOC_POSITIONS, RETAIN_HEADS * DV), 1.0, 6.0, ((0, 128),)),
    }


def reference(queries, key_vectors, values, decay_log, gate_input):
    blocks = DOC_POSITIONS // BLOCK
    query_blocks = queries.reshape(blocks, BLOCK, RETAIN_HEADS, DK)
    key_blocks = key_vectors.reshape(blocks, BLOCK, RETAIN_HEADS, DK)
    value_blocks = values.reshape(blocks, BLOCK, RETAIN_HEADS, DV)
    decay_blocks = decay_log.astype(jnp.float32).reshape(blocks, BLOCK, RETAIN_HEADS)
    causal = jnp.arange(BLOCK)[:, None] >= jnp.arange(BLOCK)[None, :]

    def advance(carried_state, pieces):
        query_block, key_block, value_block, decay_block = pieces
        running = jnp.cumsum(decay_block, axis=0)
        block_decay = running[-1]
        faded = (key_block.astype(jnp.float32) * jnp.exp(block_decay[None, :] - running)[:, :, None]).astype(jnp.bfloat16)
        state_low = carried_state.astype(jnp.bfloat16)
        spread = running.T[:, :, None] - running.T[:, None, :]
        factor = jnp.exp(jnp.where(causal[None], spread, -jnp.inf))
        scores = jnp.einsum('ihd,jhd->hij', query_block.astype(jnp.float32), key_block.astype(jnp.float32))
        weights = (scores * factor).astype(jnp.bfloat16)
        within = jnp.einsum('hij,jhw->ihw', weights.astype(jnp.float32), value_block.astype(jnp.float32))
        across = jnp.einsum('ihd,hdw->ihw', query_block.astype(jnp.float32), state_low.astype(jnp.float32))
        across = across * jnp.exp(running)[:, :, None]
        retained = (within + across).astype(jnp.bfloat16)
        additions = jnp.einsum('jhd,jhw->hdw', faded.astype(jnp.float32), value_block.astype(jnp.float32))
        updated = jnp.exp(block_decay)[:, None, None] * carried_state + additions
        return (updated, retained)
    initial = jnp.zeros((RETAIN_HEADS, DK, DV), jnp.float32)
    unused, retained = lax.scan(advance, initial, (query_blocks, key_blocks, value_blocks, decay_blocks))
    retained = retained.reshape(DOC_POSITIONS, RETAIN_HEADS, DV).astype(jnp.float32)
    average = lax.optimization_barrier(jnp.mean(retained, axis=2, keepdims=True))
    centered = retained - average
    variance = lax.optimization_barrier(jnp.mean(centered * centered, axis=2, keepdims=True))
    normed = centered / jnp.sqrt(variance + 1e-06)
    gated = jax.nn.silu(gate_input.astype(jnp.float32).reshape(DOC_POSITIONS, RETAIN_HEADS, DV)) * normed
    return gated.astype(jnp.bfloat16).reshape(DOC_POSITIONS, RETAIN_HEADS * DV)
```

```python
import jax
import jax.numpy as jnp
from jax import lax
from jax.experimental import pallas as pl
from jax.experimental.pallas import tpu as pltpu
from jax.sharding import PartitionSpec as P

MESH = pl.DeviceIdType.MESH
HEADS = 16
NH = 8
DK = 256
DV = 512
BLOCK = 512
ROWS = 256
LINES = 16
F32 = jnp.float32
BF16 = jnp.bfloat16


def remote(src, dst, send_sem, recv_sem, device):
    return pltpu.make_async_remote_copy(
        src_ref=src,
        dst_ref=dst,
        send_sem=send_sem,
        recv_sem=recv_sem,
        device_id=device,
        device_id_type=MESH,
    )


def wide(row):
    return jnp.concatenate([row] * (DV // 128), axis=1)


def body(
    q_hbm, k_hbm, v_hbm, d_hbm, g_hbm, o_hbm,
    qs, ks, vs, gs, dl,
    fadeb, runb, erunb, runt,
    abuf, r1, bk, b2s, r2, bt, r3, tt, tb, c2s, cb, s1s, sb, within, obuf,
    l_own, l_z1, l_first, l_second, l_pair, l_z2, l_p0, l_p1, l_line, l_x,
    loc, d2s, d2r, dsem, lsem, ups, upr, xs, xr, osem,
):
    x = lax.axis_index("seq")
    hd = lax.axis_index("head")
    c = lax.rem(hd, 2)
    zy = lax.div(hd, 2)
    z = lax.rem(zy, 4)
    y = lax.div(zy, 4)
    zfirst = lax.rem(z, 2) == 0
    u = lax.rem(lax.div(z + 1, 2), 2)
    w = lax.div(z, 2)
    m = x * 4 + y
    partner = (x, hd + 1 - 2 * c)
    zp1 = (x, (y * 4 + z + 1 - 2 * lax.rem(z, 2)) * 2 + c)
    zp2 = (x, (y * 4 + 3 - z) * 2 + c)

    def line_device(line):
        return (lax.div(line, 4), (lax.rem(line, 4) * 4 + z) * 2 + c)

    def slot_of(line):
        return lax.rem(line - m + 2 * LINES - 1, LINES)

    my_rows = pl.ds(pl.multiple_of(c * ROWS, ROWS), ROWS)
    other_rows = pl.ds(pl.multiple_of((1 - c) * ROWS, ROWS), ROWS)
    half_mine = pl.ds(pl.multiple_of(u * 128, 128), 128)
    half_other = pl.ds(pl.multiple_of((1 - u) * 128, 128), 128)

    big = ((k_hbm, ks, DK), (v_hbm, vs, DV), (q_hbm, qs, DK), (g_hbm, gs, DV))

    def columns(core, h, width):
        return pl.ds(pl.multiple_of((core * NH + h) * width, width), width)

    def local_in(n, h):
        src, dst, width = big[n]
        return pltpu.make_async_copy(
            src.at[:, columns(c, h, width)], dst.at[h, my_rows], loc.at[n, h]
        )

    def cross_in(n, h):
        src, dst, width = big[n]
        return remote(
            src.at[:, columns(1 - c, h, width)],
            dst.at[h, my_rows],
            d2s.at[n, h],
            d2r.at[n, h],
            partner,
        )

    def cross_arrived(n, h):
        src, dst, width = big[n]
        remote(
            src.at[:, columns(c, h, width)],
            dst.at[h, other_rows],
            d2s.at[n, h],
            d2r.at[n, h],
            partner,
        ).wait_recv()

    d_local = pltpu.make_async_copy(d_hbm, dl.at[my_rows], dsem.at[0])
    d_cross = remote(d_hbm, dl.at[my_rows], dsem.at[1], dsem.at[2], partner)

    d_local.start()

    @pl.loop(0, NH)
    def _(h):
        for n in range(4):
            local_in(n, h).start()

    barrier = pltpu.get_barrier_semaphore()
    peers = [partner, zp1, zp2] + [line_device(lax.rem(m + k, LINES)) for k in range(1, LINES)]
    for peer in peers:
        pl.semaphore_signal(barrier, inc=1, device_id=peer, device_id_type=MESH)
    pl.semaphore_wait(barrier, len(peers))

    d_cross.start()

    @pl.loop(0, NH)
    def _(h):
        cross_in(0, h).start()
        cross_in(1, h).start()

    @pl.loop(0, NH)
    def _(h):
        cross_in(2, h).start()
        cross_in(3, h).start()

    d_local.wait()
    remote(d_hbm, dl.at[other_rows], dsem.at[1], dsem.at[2], partner).wait_recv()
    row = lax.broadcasted_iota(jnp.int32, (BLOCK, BLOCK), 0)
    col = lax.broadcasted_iota(jnp.int32, (BLOCK, BLOCK), 1)
    lower = jnp.where(row >= col, 1.0, 0.0).astype(BF16)
    upper = jnp.where(row <= col, 1.0, 0.0).astype(BF16)
    decays = dl[...]
    run16 = jnp.dot(lower, decays, preferred_element_type=F32)
    runt16 = lax.dot_general(
        decays, upper, (((0,), (0,)), ((), ())), preferred_element_type=F32
    )
    run8 = jnp.where(c == 0, run16[:, :NH], run16[:, NH:])
    runt8 = jnp.where(c == 0, runt16[:NH], runt16[NH:])
    runt[...] = runt8
    last = runt8[:, BLOCK - 1 : BLOCK]
    l_own[...] = jnp.broadcast_to(last, (NH, 128))
    fade8 = jnp.exp(run8[BLOCK - 1 : BLOCK] - run8)
    erun8 = jnp.exp(run8)
    for h in range(NH):
        fadeb[h] = jnp.broadcast_to(fade8[:, h : h + 1], (BLOCK, 128))
        runb[h] = jnp.broadcast_to(run8[:, h : h + 1], (BLOCK, 128))
        erunb[h] = jnp.broadcast_to(erun8[:, h : h + 1], (BLOCK, 128))

    l1_copy = remote(l_own, l_z1, lsem.at[0], lsem.at[1], zp1)
    l2_copy = remote(l_pair, l_z2, lsem.at[2], lsem.at[3], zp2)
    l1_copy.start()

    def up1(h):
        return remote(abuf.at[h, half_other], r1.at[h], ups.at[0, h], upr.at[0, h], zp1)

    def up2(h):
        return remote(b2s.at[h], r2.at[h], ups.at[1, h], upr.at[1, h], zp2)

    def down2(h, quarter):
        rows = pl.ds(pl.multiple_of(quarter * 64, 64), 64)
        return remote(c2s.at[h], cb.at[h, rows], ups.at[2, h], upr.at[2, h], zp2)

    def down1(h, rows):
        return remote(s1s.at[h], sb.at[h, rows], ups.at[3, h], upr.at[3, h], zp1)

    def x_send(h, k):
        line = lax.rem(m + k, LINES)
        return remote(
            bt.at[h, line],
            r3.at[h, LINES - 1 - k],
            xs.at[0, h],
            xr.at[0, h],
            line_device(line),
        )

    def y_send(h, k):
        line = lax.rem(m + k, LINES)
        return remote(
            tt.at[h, k - 1],
            tb.at[h, LINES - 1 - k],
            xs.at[1, h],
            xr.at[1, h],
            line_device(line),
        )

    def all_lines(buffer, n, h):
        some = buffer.at[h, pl.ds(0, LINES - 1)]
        return remote(some, some, xs.at[n, h], xr.at[n, h], zp1)

    @pl.loop(0, NH)
    def _(h):
        for n in range(2):
            local_in(n, h).wait()
            cross_arrived(n, h)
        fade = fadeb[h]
        faded = (ks[h].astype(F32) * jnp.concatenate([fade, fade], axis=1)).astype(BF16)
        addition = lax.dot_general(
            faded, vs[h], (((0,), (0,)), ((), ())), preferred_element_type=F32
        )
        abuf[h] = addition.astype(BF16)
        up1(h).start()

    l1_copy.wait_recv()
    mine, got = l_own[...], l_z1[...]
    l_first[...] = jnp.where(zfirst, mine, got)
    l_second[...] = jnp.where(zfirst, got, mine)
    l_pair[...] = mine + got
    l2_copy.start()

    def exp_row(ref, h):
        return jnp.exp(ref[pl.ds(h, 1), :])

    def combine_pair(h):
        up1(h).wait_recv()
        rate = wide(exp_row(l_second, h))
        one = jnp.ones_like(rate)
        rate_mine = jnp.where(zfirst, rate, one)
        rate_got = jnp.where(zfirst, one, rate)

        def total(quarter):
            at = pl.multiple_of(quarter * 64, 64)
            a = abuf[h, pl.ds(pl.multiple_of(u * 128 + at, 64), 64), :].astype(F32)
            b = r1[h, pl.ds(at, 64), :].astype(F32)
            return rate_mine * a + rate_got * b

        b2s[h] = total(1 - w).astype(BF16)
        up2(h).start()
        bk[h] = total(w)

    def share_rates():
        l2_copy.wait_recv()
        own_pair, got_pair = l_pair[...], l_z2[...]
        l_p0[...] = jnp.where(w == 0, own_pair, got_pair)
        l_p1[...] = jnp.where(w == 0, got_pair, own_pair)
        total = own_pair + got_pair
        l_line[...] = total
        l_x[LINES - 1] = total
        for k in range(1, LINES):
            remote(
                l_line,
                l_x.at[LINES - 1 - k],
                lsem.at[4],
                lsem.at[5],
                line_device(lax.rem(m + k, LINES)),
            ).start()

    rates_wait = remote(
        l_x.at[pl.ds(0, LINES - 1)], l_x.at[pl.ds(0, LINES - 1)], lsem.at[4], lsem.at[5], zp1
    )

    def combine_line(h):
        up2(h).wait_recv()
        rate = wide(exp_row(l_p1, h))
        one = jnp.ones_like(rate)
        total = jnp.where(w == 0, rate, one) * bk[h] + jnp.where(w == 0, one, rate) * r2[h].astype(F32)
        low = total.astype(BF16)
        for line in range(LINES):
            r, s = 16 * (line // 4), 128 * (line % 4)
            bt[h, line] = low[r : r + 16, s : s + 128]
        for k in range(1, LINES):
            x_send(h, k).start()
        r3[h, LINES - 1] = bt[h, m]

    def scan_lines(h):
        all_lines(r3, 0, h).wait_recv()
        carry = jnp.zeros((16, 128), F32)
        for line in range(LINES):
            slot = slot_of(line)
            low = carry.astype(BF16)
            tt[h, slot] = low
            if line < LINES - 1:
                rate = jnp.exp(l_x[slot, pl.ds(h, 1), :])
                carry = rate * carry + r3[h, slot].astype(F32)
        for k in range(1, LINES):
            y_send(h, k).start()
        tb[h, LINES - 1] = tt[h, LINES - 1]

    def carry_pairs(h):
        all_lines(tb, 1, h).wait_recv()
        rate = exp_row(l_p0, h)
        base = w * 64
        for line in range(LINES):
            r, s = 16 * (line // 4), 128 * (line % 4)
            start = tb[h, slot_of(line)].astype(F32)
            first_pair = jnp.where(
                w == 0, bk[h, r : r + 16, s : s + 128], r2[h, r : r + 16, s : s + 128].astype(F32)
            )
            after = rate * start + first_pair
            rows = pl.ds(pl.multiple_of(base + r, 16), 16)
            c2s[h, r : r + 16, s : s + 128] = jnp.where(w == 0, after, start).astype(BF16)
            cb[h, rows, s : s + 128] = jnp.where(w == 0, start, after).astype(BF16)
        down2(h, w).start()

    def carry_chips(h):
        down2(h, 1 - w).wait_recv()
        rate = wide(exp_row(l_first, h))
        for r in (0, 64):
            start = cb[h, r : r + 64, :].astype(F32)
            own_rows = pl.ds(pl.multiple_of(u * 128 + r, 64), 64)
            addition = jnp.where(zfirst, abuf[h, own_rows, :], r1[h, r : r + 64, :])
            after = rate * start + addition.astype(F32)
            s1s[h, r : r + 64, :] = jnp.where(zfirst, after, start).astype(BF16)
            sb[h, own_rows, :] = jnp.where(zfirst, start, after).astype(BF16)
        down1(h, half_mine).start()

    def within_block(h):
        local_in(2, h).wait()
        cross_arrived(2, h)
        for tile in range(2):
            keys = ROWS * (tile + 1)
            rows = slice(ROWS * tile, ROWS * (tile + 1))
            scores = lax.dot_general(
                qs[h, rows, :],
                ks[h, :keys, :],
                (((1,), (1,)), ((), ())),
                preferred_element_type=F32,
            )
            left = runb[h, rows, :]
            spread = jnp.concatenate([left] * (keys // 128), axis=1) - runt[pl.ds(h, 1), :keys]
            i = lax.broadcasted_iota(jnp.int32, (ROWS, keys), 0) + ROWS * tile
            j = lax.broadcasted_iota(jnp.int32, (ROWS, keys), 1)
            factor = jnp.exp(jnp.where(i >= j, spread, -jnp.inf))
            weights = (scores * factor).astype(BF16)
            within[h, rows, :] = jnp.dot(weights, vs[h, :keys, :], preferred_element_type=F32)

    def out_local(h):
        return pltpu.make_async_copy(
            obuf.at[h, my_rows], o_hbm.at[:, columns(c, h, DV)], osem.at[0, h]
        )

    def out_cross(h, core):
        return remote(
            obuf.at[h, other_rows],
            o_hbm.at[:, columns(core, h, DV)],
            osem.at[1, h],
            osem.at[2, h],
            partner,
        )

    def finish(h):
        local_in(3, h).wait()
        cross_arrived(3, h)
        down1(h, half_other).wait_recv()
        state = sb[h]
        for tile in range(4):
            rows = slice(128 * tile, 128 * (tile + 1))
            across = jnp.dot(qs[h, rows, :], state, preferred_element_type=F32)
            retained = within[h, rows, :] + across * wide(erunb[h, rows, :])
            retained = retained.astype(BF16).astype(F32)
            centered = retained - jnp.mean(retained, axis=1, keepdims=True)
            variance = jnp.mean(centered * centered, axis=1, keepdims=True)
            normed = centered * lax.rsqrt(variance + 1e-6)
            gate = gs[h, rows, :].astype(F32)
            gated = gate / (1.0 + jnp.exp(-gate)) * normed
            obuf[h, rows, :] = gated.astype(BF16)
        out_cross(h, c).start()
        out_local(h).start()

    @pl.loop(0, 2 * NH)
    def _(t):
        def stage(lag, f):
            @pl.when((t >= lag) & (t < lag + NH))
            def _():
                f(t - lag)

        stage(0, combine_pair)

        @pl.when(t == 0)
        def _():
            share_rates()

        stage(8, finish)
        stage(1, combine_line)
        stage(4, carry_pairs)
        stage(5, carry_chips)

        @pl.when(t == 2)
        def _():
            rates_wait.wait_recv()

        stage(2, scan_lines)
        stage(0, within_block)

    d_cross.wait_send()
    l1_copy.wait_send()
    l2_copy.wait_send()
    rates_wait.wait_send()

    @pl.loop(0, NH)
    def _(h):
        for n in range(4):
            cross_in(n, h).wait_send()
        up1(h).wait_send()
        up2(h).wait_send()
        down2(h, w).wait_send()
        down1(h, half_mine).wait_send()
        all_lines(r3, 0, h).wait_send()
        all_lines(tb, 1, h).wait_send()
        out_local(h).wait()
        out_cross(h, c).wait_send()
        out_cross(h, 1 - c).wait_recv()


def shards(queries, key_vectors, values, decay_log, gate_input):
    anywhere = pl.BlockSpec(memory_space=pl.ANY)
    tile = pltpu.VMEM((NH, 128), F32)
    dma = pltpu.SemaphoreType.DMA
    return pl.pallas_call(
        body,
        out_shape=jax.ShapeDtypeStruct((ROWS, HEADS * DV), BF16),
        in_specs=[anywhere] * 5,
        out_specs=anywhere,
        scratch_shapes=[
            pltpu.VMEM((NH, BLOCK, DK), BF16),
            pltpu.VMEM((NH, BLOCK, DK), BF16),
            pltpu.VMEM((NH, BLOCK, DV), BF16),
            pltpu.VMEM((NH, BLOCK, DV), BF16),
            pltpu.VMEM((BLOCK, HEADS), BF16),
            pltpu.VMEM((NH, BLOCK, 128), F32),
            pltpu.VMEM((NH, BLOCK, 128), F32),
            pltpu.VMEM((NH, BLOCK, 128), F32),
            pltpu.VMEM((NH, BLOCK), F32),
            pltpu.VMEM((NH, DK, DV), BF16),
            pltpu.VMEM((NH, 128, DV), BF16),
            pltpu.VMEM((NH, 64, DV), F32),
            pltpu.VMEM((NH, 64, DV), BF16),
            pltpu.VMEM((NH, 64, DV), BF16),
            pltpu.VMEM((NH, LINES, 16, 128), BF16),
            pltpu.VMEM((NH, LINES, 16, 128), BF16),
            pltpu.VMEM((NH, LINES, 16, 128), BF16),
            pltpu.VMEM((NH, LINES, 16, 128), BF16),
            pltpu.VMEM((NH, 64, DV), BF16),
            pltpu.VMEM((NH, 128, DV), BF16),
            pltpu.VMEM((NH, 128, DV), BF16),
            pltpu.VMEM((NH, DK, DV), BF16),
            pltpu.VMEM((NH, BLOCK, DV), F32),
            pltpu.VMEM((NH, BLOCK, DV), BF16),
            *[tile] * 9,
            pltpu.VMEM((LINES, NH, 128), F32),
            dma((4, NH)),
            dma((4, NH)),
            dma((4, NH)),
            dma((3,)),
            dma((6,)),
            dma((4, NH)),
            dma((4, NH)),
            dma((2, NH)),
            dma((2, NH)),
            dma((3, NH)),
        ],
        compiler_params=pltpu.CompilerParams(
            collective_id=0, has_side_effects=True, vmem_limit_bytes=60 * 1024 * 1024
        ),
        name="retention",
    )(queries, key_vectors, values, decay_log, gate_input)


def solution(mesh):
    spec = P(("seq", "head"), None)
    return jax.shard_map(
        shards, mesh=mesh, in_specs=(spec,) * 5, out_specs=spec, check_vma=False
    )
```

```python
import jax
import jax.numpy as jnp
from jax import lax
from jax.experimental import pallas as pl
from jax.experimental.pallas import tpu as pltpu
from jax.sharding import PartitionSpec as P

MESH = pl.DeviceIdType.MESH
HEADS = 16
NH = 8
DK = 256
DV = 512
BLOCK = 512
ROWS = 256
LINES = 16
F32 = jnp.float32
BF16 = jnp.bfloat16
VMEM = 52 * 1024 * 1024


def remote(src, dst, send_sem, recv_sem, device):
    return pltpu.make_async_remote_copy(
        src_ref=src,
        dst_ref=dst,
        send_sem=send_sem,
        recv_sem=recv_sem,
        device_id=device,
        device_id_type=MESH,
    )


def wide(row):
    return jnp.concatenate([row] * (DV // 128), axis=1)


def body(
    q_hbm, k_hbm, v_hbm, d_hbm, g_hbm, o_hbm,
    qs, ks, vs, gs, dl,
    fadeb, runb, erunb, runt,
    abuf, r1, bk, b2s, r2, bt, r3, tt, tb, c2s, cb, s1s, sb, within, obuf,
    l_own, l_z1, l_first, l_second, l_pair, l_z2, l_p0, l_p1, l_line, l_x,
    loc, d2s, d2r, dsem, lsem, ups, upr, xs, xr, osem,
):
    x = lax.axis_index("seq")
    hd = lax.axis_index("head")
    c = lax.rem(hd, 2)
    zy = lax.div(hd, 2)
    z = lax.rem(zy, 4)
    y = lax.div(zy, 4)
    zfirst = lax.rem(z, 2) == 0
    u = lax.rem(lax.div(z + 1, 2), 2)
    w = lax.div(z, 2)
    m = x * 4 + y
    partner = (x, hd + 1 - 2 * c)
    zp1 = (x, (y * 4 + z + 1 - 2 * lax.rem(z, 2)) * 2 + c)
    zp2 = (x, (y * 4 + 3 - z) * 2 + c)

    def line_device(line):
        return (lax.div(line, 4), (lax.rem(line, 4) * 4 + z) * 2 + c)

    def slot_of(line):
        return lax.rem(line - m + 2 * LINES - 1, LINES)

    my_rows = pl.ds(pl.multiple_of(c * ROWS, ROWS), ROWS)
    other_rows = pl.ds(pl.multiple_of((1 - c) * ROWS, ROWS), ROWS)
    half_mine = pl.ds(pl.multiple_of(u * 128, 128), 128)
    half_other = pl.ds(pl.multiple_of((1 - u) * 128, 128), 128)

    big = ((k_hbm, ks, DK), (v_hbm, vs, DV), (q_hbm, qs, DK), (g_hbm, gs, DV))

    def columns(core, h, width):
        return pl.ds(pl.multiple_of((core * NH + h) * width, width), width)

    def local_in(n, h):
        src, dst, width = big[n]
        return pltpu.make_async_copy(
            src.at[:, columns(c, h, width)], dst.at[h, my_rows], loc.at[n, h]
        )

    def cross_in(n, h):
        src, dst, width = big[n]
        return remote(
            src.at[:, columns(1 - c, h, width)],
            dst.at[h, my_rows],
            d2s.at[n, h],
            d2r.at[n, h],
            partner,
        )

    def cross_arrived(n, h):
        src, dst, width = big[n]
        remote(
            src.at[:, columns(c, h, width)],
            dst.at[h, other_rows],
            d2s.at[n, h],
            d2r.at[n, h],
            partner,
        ).wait_recv()

    d_local = pltpu.make_async_copy(d_hbm, dl.at[:, my_rows], dsem.at[0])
    d_cross = remote(d_hbm, dl.at[:, my_rows], dsem.at[1], dsem.at[2], partner)

    d_local.start()

    @pl.loop(0, NH)
    def _(h):
        for n in range(4):
            local_in(n, h).start()

    barrier = pltpu.get_barrier_semaphore()
    peers = [partner, zp1, zp2] + [line_device(lax.rem(m + k, LINES)) for k in range(1, LINES)]
    for peer in peers:
        pl.semaphore_signal(barrier, inc=1, device_id=peer, device_id_type=MESH)
    pl.semaphore_wait(barrier, len(peers))

    d_cross.start()

    @pl.loop(0, NH)
    def _(h):
        cross_in(0, h).start()
        cross_in(1, h).start()

    @pl.loop(0, NH)
    def _(h):
        cross_in(2, h).start()
        cross_in(3, h).start()

    d_local.wait()
    remote(d_hbm, dl.at[:, other_rows], dsem.at[1], dsem.at[2], partner).wait_recv()
    row = lax.broadcasted_iota(jnp.int32, (BLOCK, BLOCK), 0)
    col = lax.broadcasted_iota(jnp.int32, (BLOCK, BLOCK), 1)
    lower = jnp.where(row >= col, 1.0, 0.0).astype(BF16)
    upper = jnp.where(row <= col, 1.0, 0.0).astype(BF16)
    decays = dl[...]
    run16 = lax.dot_general(
        lower, decays, (((1,), (1,)), ((), ())), preferred_element_type=F32
    )
    runt16 = jnp.dot(decays, upper, preferred_element_type=F32)
    run8 = jnp.where(c == 0, run16[:, :NH], run16[:, NH:])
    runt8 = jnp.where(c == 0, runt16[:NH], runt16[NH:])
    runt[...] = runt8
    last = runt8[:, BLOCK - 1 : BLOCK]
    l_own[...] = jnp.broadcast_to(last, (NH, 128))
    fade8 = jnp.exp(run8[BLOCK - 1 : BLOCK] - run8)
    erun8 = jnp.exp(run8)
    for h in range(NH):
        fadeb[h] = jnp.broadcast_to(fade8[:, h : h + 1], (BLOCK, 128))
        runb[h] = jnp.broadcast_to(run8[:, h : h + 1], (BLOCK, 128))
        erunb[h] = jnp.broadcast_to(erun8[:, h : h + 1], (BLOCK, 128))

    l1_copy = remote(l_own, l_z1, lsem.at[0], lsem.at[1], zp1)
    l2_copy = remote(l_pair, l_z2, lsem.at[2], lsem.at[3], zp2)
    l1_copy.start()

    def up1(h):
        return remote(abuf.at[h, half_other], r1.at[h], ups.at[0, h], upr.at[0, h], zp1)

    def up2(h):
        return remote(b2s.at[h], r2.at[h], ups.at[1, h], upr.at[1, h], zp2)

    def down2(h, quarter):
        rows = pl.ds(pl.multiple_of(quarter * 64, 64), 64)
        return remote(c2s.at[h], cb.at[h, rows], ups.at[2, h], upr.at[2, h], zp2)

    def down1(h, rows):
        return remote(s1s.at[h], sb.at[h, rows], ups.at[3, h], upr.at[3, h], zp1)

    def x_send(h, k):
        line = lax.rem(m + k, LINES)
        return remote(
            bt.at[h, line],
            r3.at[h, LINES - 1 - k],
            xs.at[0, h],
            xr.at[0, h],
            line_device(line),
        )

    def y_send(h, k):
        line = lax.rem(m + k, LINES)
        return remote(
            tt.at[h, k - 1],
            tb.at[h, LINES - 1 - k],
            xs.at[1, h],
            xr.at[1, h],
            line_device(line),
        )

    def all_lines(buffer, n, h):
        some = buffer.at[h, pl.ds(0, LINES - 1)]
        return remote(some, some, xs.at[n, h], xr.at[n, h], zp1)

    @pl.loop(0, NH)
    def _(h):
        for n in range(2):
            local_in(n, h).wait()
            cross_arrived(n, h)
        fade = fadeb[h]
        faded = (ks[h].astype(F32) * jnp.concatenate([fade, fade], axis=1)).astype(BF16)
        addition = lax.dot_general(
            faded, vs[h], (((0,), (0,)), ((), ())), preferred_element_type=F32
        )
        abuf[h] = addition.astype(BF16)
        up1(h).start()

    l1_copy.wait_recv()
    mine, got = l_own[...], l_z1[...]
    l_first[...] = jnp.where(zfirst, mine, got)
    l_second[...] = jnp.where(zfirst, got, mine)
    l_pair[...] = mine + got
    l2_copy.start()

    def exp_row(ref, h):
        return jnp.exp(ref[pl.ds(h, 1), :])

    def combine_pair(h):
        up1(h).wait_recv()
        rate = wide(exp_row(l_second, h))
        one = jnp.ones_like(rate)
        rate_mine = jnp.where(zfirst, rate, one)
        rate_got = jnp.where(zfirst, one, rate)

        def total(quarter):
            at = pl.multiple_of(quarter * 64, 64)
            a = abuf[h, pl.ds(pl.multiple_of(u * 128 + at, 64), 64), :].astype(F32)
            b = r1[h, pl.ds(at, 64), :].astype(F32)
            return rate_mine * a + rate_got * b

        b2s[h] = total(1 - w).astype(BF16)
        up2(h).start()
        bk[h] = total(w)

    def share_rates():
        l2_copy.wait_recv()
        own_pair, got_pair = l_pair[...], l_z2[...]
        l_p0[...] = jnp.where(w == 0, own_pair, got_pair)
        l_p1[...] = jnp.where(w == 0, got_pair, own_pair)
        total = own_pair + got_pair
        l_line[...] = total
        l_x[LINES - 1] = total
        for k in range(1, LINES):
            remote(
                l_line,
                l_x.at[LINES - 1 - k],
                lsem.at[4],
                lsem.at[5],
                line_device(lax.rem(m + k, LINES)),
            ).start()

    rates_wait = remote(
        l_x.at[pl.ds(0, LINES - 1)], l_x.at[pl.ds(0, LINES - 1)], lsem.at[4], lsem.at[5], zp1
    )

    def combine_line(h):
        up2(h).wait_recv()
        rate = wide(exp_row(l_p1, h))
        one = jnp.ones_like(rate)
        total = jnp.where(w == 0, rate, one) * bk[h] + jnp.where(w == 0, one, rate) * r2[h].astype(F32)
        low = total.astype(BF16)
        for line in range(LINES):
            r, s = 16 * (line // 4), 128 * (line % 4)
            bt[h, line] = low[r : r + 16, s : s + 128]
        for k in range(1, LINES):
            x_send(h, k).start()
        r3[h, LINES - 1] = bt[h, m]

    def scan_lines(h):
        all_lines(r3, 0, h).wait_recv()
        carry = jnp.zeros((16, 128), F32)
        for line in range(LINES):
            slot = slot_of(line)
            low = carry.astype(BF16)
            tt[h, slot] = low
            if line < LINES - 1:
                rate = jnp.exp(l_x[slot, pl.ds(h, 1), :])
                carry = rate * carry + r3[h, slot].astype(F32)
        for k in range(1, LINES):
            y_send(h, k).start()
        tb[h, LINES - 1] = tt[h, LINES - 1]

    def carry_pairs(h):
        all_lines(tb, 1, h).wait_recv()
        rate = exp_row(l_p0, h)
        base = w * 64
        for line in range(LINES):
            r, s = 16 * (line // 4), 128 * (line % 4)
            start = tb[h, slot_of(line)].astype(F32)
            first_pair = jnp.where(
                w == 0, bk[h, r : r + 16, s : s + 128], r2[h, r : r + 16, s : s + 128].astype(F32)
            )
            after = rate * start + first_pair
            rows = pl.ds(pl.multiple_of(base + r, 16), 16)
            c2s[h, r : r + 16, s : s + 128] = jnp.where(w == 0, after, start).astype(BF16)
            cb[h, rows, s : s + 128] = jnp.where(w == 0, start, after).astype(BF16)
        down2(h, w).start()

    def carry_chips(h):
        down2(h, 1 - w).wait_recv()
        rate = wide(exp_row(l_first, h))
        for r in (0, 64):
            start = cb[h, r : r + 64, :].astype(F32)
            own_rows = pl.ds(pl.multiple_of(u * 128 + r, 64), 64)
            addition = jnp.where(zfirst, abuf[h, own_rows, :], r1[h, r : r + 64, :])
            after = rate * start + addition.astype(F32)
            s1s[h, r : r + 64, :] = jnp.where(zfirst, after, start).astype(BF16)
            sb[h, own_rows, :] = jnp.where(zfirst, start, after).astype(BF16)
        down1(h, half_mine).start()

    def within_block(h):
        local_in(2, h).wait()
        cross_arrived(2, h)
        for tile in range(2):
            keys = ROWS * (tile + 1)
            rows = slice(ROWS * tile, ROWS * (tile + 1))
            scores = lax.dot_general(
                qs[h, rows, :],
                ks[h, :keys, :],
                (((1,), (1,)), ((), ())),
                preferred_element_type=F32,
            )
            left = runb[h, rows, :]
            spread = jnp.concatenate([left] * (keys // 128), axis=1) - runt[pl.ds(h, 1), :keys]
            i = lax.broadcasted_iota(jnp.int32, (ROWS, keys), 0) + ROWS * tile
            j = lax.broadcasted_iota(jnp.int32, (ROWS, keys), 1)
            factor = jnp.exp(jnp.where(i >= j, spread, -jnp.inf))
            weights = (scores * factor).astype(BF16)
            within[h, rows, :] = jnp.dot(weights, vs[h, :keys, :], preferred_element_type=F32)

    def out_local(h):
        return pltpu.make_async_copy(
            obuf.at[h, my_rows], o_hbm.at[:, columns(c, h, DV)], osem.at[0, h]
        )

    def out_cross(h, core):
        return remote(
            obuf.at[h, other_rows],
            o_hbm.at[:, columns(core, h, DV)],
            osem.at[1, h],
            osem.at[2, h],
            partner,
        )

    def finish(h):
        local_in(3, h).wait()
        cross_arrived(3, h)
        down1(h, half_other).wait_recv()
        state = sb[h]
        for tile in range(4):
            rows = slice(128 * tile, 128 * (tile + 1))
            across = jnp.dot(qs[h, rows, :], state, preferred_element_type=F32)
            retained = within[h, rows, :] + across * wide(erunb[h, rows, :])
            retained = retained.astype(BF16).astype(F32)
            centered = retained - jnp.mean(retained, axis=1, keepdims=True)
            variance = jnp.mean(centered * centered, axis=1, keepdims=True)
            normed = centered * lax.rsqrt(variance + 1e-6)
            gate = gs[h, rows, :].astype(F32)
            gated = gate / (1.0 + jnp.exp(-gate)) * normed
            obuf[h, rows, :] = gated.astype(BF16)
        out_cross(h, c).start()
        out_local(h).start()

    @pl.loop(0, NH + 8)
    def _(t):
        def stage(lag, f):
            @pl.when((t >= lag) & (t < lag + NH))
            def _():
                f(t - lag)

        stage(0, combine_pair)

        @pl.when(t == 0)
        def _():
            share_rates()

        stage(6, carry_chips)

        @pl.when(t == 3)
        def _():
            rates_wait.wait_recv()

        stage(3, scan_lines)
        stage(8, finish)
        stage(1, combine_line)
        stage(4, carry_pairs)
        stage(0, within_block)

    d_cross.wait_send()
    l1_copy.wait_send()
    l2_copy.wait_send()
    rates_wait.wait_send()

    @pl.loop(0, NH)
    def _(h):
        for n in range(4):
            cross_in(n, h).wait_send()
        up1(h).wait_send()
        up2(h).wait_send()
        down2(h, w).wait_send()
        down1(h, half_mine).wait_send()
        all_lines(r3, 0, h).wait_send()
        all_lines(tb, 1, h).wait_send()
        out_local(h).wait()
        out_cross(h, c).wait_send()
        out_cross(h, 1 - c).wait_recv()


def shards(queries, key_vectors, values, decay_log, gate_input):
    anywhere = pl.BlockSpec(memory_space=pl.ANY)
    tile = pltpu.VMEM((NH, 128), F32)
    dma = pltpu.SemaphoreType.DMA
    return pl.pallas_call(
        body,
        out_shape=pltpu.VMEM((ROWS, HEADS * DV), BF16),
        in_specs=[anywhere] * 5,
        out_specs=pl.BlockSpec(memory_space=pltpu.VMEM),
        scratch_shapes=[
            pltpu.VMEM((NH, BLOCK, DK), BF16),
            pltpu.VMEM((NH, BLOCK, DK), BF16),
            pltpu.VMEM((NH, BLOCK, DV), BF16),
            pltpu.VMEM((NH, BLOCK, DV), BF16),
            pltpu.VMEM((HEADS, BLOCK), BF16),
            pltpu.VMEM((NH, BLOCK, 128), F32),
            pltpu.VMEM((NH, BLOCK, 128), F32),
            pltpu.VMEM((NH, BLOCK, 128), F32),
            pltpu.VMEM((NH, BLOCK), F32),
            pltpu.VMEM((NH, DK, DV), BF16),
            pltpu.VMEM((NH, 128, DV), BF16),
            pltpu.VMEM((NH, 64, DV), F32),
            pltpu.VMEM((NH, 64, DV), BF16),
            pltpu.VMEM((NH, 64, DV), BF16),
            pltpu.VMEM((NH, LINES, 16, 128), BF16),
            pltpu.VMEM((NH, LINES, 16, 128), BF16),
            pltpu.VMEM((NH, LINES, 16, 128), BF16),
            pltpu.VMEM((NH, LINES, 16, 128), BF16),
            pltpu.VMEM((NH, 64, DV), BF16),
            pltpu.VMEM((NH, 128, DV), BF16),
            pltpu.VMEM((NH, 128, DV), BF16),
            pltpu.VMEM((NH, DK, DV), BF16),
            pltpu.VMEM((NH, BLOCK, DV), F32),
            pltpu.VMEM((NH, BLOCK, DV), BF16),
            *[tile] * 9,
            pltpu.VMEM((LINES, NH, 128), F32),
            dma((4, NH)),
            dma((4, NH)),
            dma((4, NH)),
            dma((3,)),
            dma((6,)),
            dma((4, NH)),
            dma((4, NH)),
            dma((2, NH)),
            dma((2, NH)),
            dma((3, NH)),
        ],
        compiler_params=pltpu.CompilerParams(
            collective_id=0, has_side_effects=True, vmem_limit_bytes=VMEM
        ),
        name="retention",
    )(queries, key_vectors, values, decay_log.T, gate_input)


def solution(mesh):
    spec = P(("seq", "head"), None)
    return jax.shard_map(
        shards, mesh=mesh, in_specs=(spec,) * 5, out_specs=spec, check_vma=False
    )
```

```python
import jax
import jax.numpy as jnp
from jax import lax
from jax.experimental import pallas as pl
from jax.experimental.pallas import tpu as pltpu
from jax.sharding import PartitionSpec as P

MESH = pl.DeviceIdType.MESH
HEADS = 16
NH = 8
DK = 256
DV = 512
BLOCK = 512
ROWS = 256
LINES = 16
F32 = jnp.float32
BF16 = jnp.bfloat16
VMEM = 52 * 1024 * 1024


def remote(src, dst, send_sem, recv_sem, device):
    return pltpu.make_async_remote_copy(
        src_ref=src,
        dst_ref=dst,
        send_sem=send_sem,
        recv_sem=recv_sem,
        device_id=device,
        device_id_type=MESH,
    )


def wide(row):
    return jnp.concatenate([row] * (DV // 128), axis=1)


def body(
    q_hbm, k_hbm, v_hbm, d_hbm, g_hbm, o_ref,
    qs, ks, vs, gs, dl,
    fadeb, runb, erunb, runt,
    abuf, r1, bk, b2s, r2, bt, r3, tt, tb, c2s, cb, s1s, sb, within, obuf,
    l_own, l_z1, l_first, l_second, l_pair, l_z2, l_p0, l_p1, l_line, l_x,
    loc, d2s, d2r, dsem, lsem, ups, upr, xs, xr, osem,
):
    x = lax.axis_index("seq")
    hd = lax.axis_index("head")
    c = lax.rem(hd, 2)
    zy = lax.div(hd, 2)
    z = lax.rem(zy, 4)
    y = lax.div(zy, 4)
    zfirst = lax.rem(z, 2) == 0
    u = lax.rem(lax.div(z + 1, 2), 2)
    w = lax.div(z, 2)
    m = x * 4 + y
    partner = (x, hd + 1 - 2 * c)
    zp1 = (x, (y * 4 + z + 1 - 2 * lax.rem(z, 2)) * 2 + c)
    zp2 = (x, (y * 4 + 3 - z) * 2 + c)

    def line_device(line):
        return (lax.div(line, 4), (lax.rem(line, 4) * 4 + z) * 2 + c)

    def slot_of(line):
        return lax.rem(line - m + 2 * LINES - 1, LINES)

    my_rows = pl.ds(pl.multiple_of(c * ROWS, ROWS), ROWS)
    other_rows = pl.ds(pl.multiple_of((1 - c) * ROWS, ROWS), ROWS)
    half_mine = pl.ds(pl.multiple_of(u * 128, 128), 128)
    half_other = pl.ds(pl.multiple_of((1 - u) * 128, 128), 128)

    big = ((k_hbm, ks, DK), (v_hbm, vs, DV), (q_hbm, qs, DK), (g_hbm, gs, DV))

    def columns(core, h, width):
        return pl.ds(pl.multiple_of((core * NH + h) * width, width), width)

    def arrival(sems, n, h):
        return sems.at[n, h] if n < 2 else sems.at[n, 0]

    def local_in(n, h):
        src, dst, width = big[n]
        return pltpu.make_async_copy(
            src.at[:, columns(c, h, width)], dst.at[h, my_rows], arrival(loc, n, h)
        )

    def cross_in(n, h):
        src, dst, width = big[n]
        return remote(
            src.at[:, columns(1 - c, h, width)],
            dst.at[h, my_rows],
            d2s.at[n],
            arrival(d2r, n, h),
            partner,
        )

    def cross_arrived(n, h):
        dst = big[n][1].at[h, other_rows]
        remote(dst, dst, d2s.at[n], arrival(d2r, n, h), partner).wait_recv()

    def all_arrived(n):
        own, got = big[n][1].at[:, my_rows], big[n][1].at[:, other_rows]
        pltpu.make_async_copy(own, own, loc.at[n, 0]).wait()
        remote(got, got, d2s.at[n], d2r.at[n, 0], partner).wait_recv()

    d_local = pltpu.make_async_copy(d_hbm, dl.at[:, my_rows], dsem.at[0])
    d_cross = remote(d_hbm, dl.at[:, my_rows], dsem.at[1], dsem.at[2], partner)

    d_local.start()

    @pl.loop(0, NH)
    def _(h):
        for n in range(2):
            local_in(n, h).start()

    barrier = pltpu.get_barrier_semaphore()
    peers = [partner, zp1, zp2] + [line_device(lax.rem(m + k, LINES)) for k in range(1, LINES)]
    for peer in peers:
        pl.semaphore_signal(barrier, inc=1, device_id=peer, device_id_type=MESH)
    pl.semaphore_wait(barrier, len(peers))

    d_cross.start()

    @pl.loop(0, NH)
    def _(h):
        cross_in(0, h).start()
        cross_in(1, h).start()

    @pl.loop(0, NH)
    def _(h):
        for n in (2, 3):
            local_in(n, h).start()
            cross_in(n, h).start()

    d_local.wait()
    remote(d_hbm, dl.at[:, other_rows], dsem.at[1], dsem.at[2], partner).wait_recv()
    row = lax.broadcasted_iota(jnp.int32, (BLOCK, BLOCK), 0)
    col = lax.broadcasted_iota(jnp.int32, (BLOCK, BLOCK), 1)
    lower = jnp.where(row >= col, 1.0, 0.0).astype(BF16)
    upper = jnp.where(row <= col, 1.0, 0.0).astype(BF16)
    decays = dl[...]
    run16 = lax.dot_general(
        lower, decays, (((1,), (1,)), ((), ())), preferred_element_type=F32
    )
    runt16 = jnp.dot(decays, upper, preferred_element_type=F32)
    run8 = jnp.where(c == 0, run16[:, :NH], run16[:, NH:])
    runt8 = jnp.where(c == 0, runt16[:NH], runt16[NH:])
    runt[...] = runt8
    last = runt8[:, BLOCK - 1 : BLOCK]
    l_own[...] = jnp.broadcast_to(last, (NH, 128))
    fade8 = jnp.exp(run8[BLOCK - 1 : BLOCK] - run8)
    erun8 = jnp.exp(run8)
    for h in range(NH):
        fadeb[h] = jnp.broadcast_to(fade8[:, h : h + 1], (BLOCK, 128))
        runb[h] = jnp.broadcast_to(run8[:, h : h + 1], (BLOCK, 128))
        erunb[h] = jnp.broadcast_to(erun8[:, h : h + 1], (BLOCK, 128))

    l1_copy = remote(l_own, l_z1, lsem.at[0], lsem.at[1], zp1)
    l2_copy = remote(l_pair, l_z2, lsem.at[2], lsem.at[3], zp2)
    l1_copy.start()

    def up1(h):
        return remote(abuf.at[h, half_other], r1.at[h], ups.at[0], upr.at[0, h], zp1)

    def up2(h):
        return remote(b2s.at[h], r2.at[h], ups.at[1], upr.at[1, h], zp2)

    def down2(h, quarter):
        rows = pl.ds(pl.multiple_of(quarter * 64, 64), 64)
        return remote(c2s.at[h], cb.at[h, rows], ups.at[2], upr.at[2, h], zp2)

    def down1(h, rows):
        return remote(s1s.at[h], sb.at[h, rows], ups.at[3], upr.at[3, h], zp1)

    def x_send(h, k):
        line = lax.rem(m + k, LINES)
        return remote(
            bt.at[h, line],
            r3.at[h, LINES - 1 - k],
            xs.at[0],
            xr.at[0, h],
            line_device(line),
        )

    def y_send(h, k):
        line = lax.rem(m + k, LINES)
        return remote(
            tt.at[h, k - 1],
            tb.at[h, LINES - 1 - k],
            xs.at[1],
            xr.at[1, h],
            line_device(line),
        )

    def all_lines(buffer, n, h):
        some = buffer.at[h, pl.ds(0, LINES - 1)]
        return remote(some, some, xs.at[n], xr.at[n, h], zp1)

    @pl.loop(0, NH)
    def _(h):
        for n in range(2):
            local_in(n, h).wait()
            cross_arrived(n, h)
        fade = fadeb[h]
        faded = (ks[h].astype(F32) * jnp.concatenate([fade, fade], axis=1)).astype(BF16)
        addition = lax.dot_general(
            faded, vs[h], (((0,), (0,)), ((), ())), preferred_element_type=F32
        )
        abuf[h] = addition.astype(BF16)
        up1(h).start()

    l1_copy.wait_recv()
    mine, got = l_own[...], l_z1[...]
    l_first[...] = jnp.where(zfirst, mine, got)
    l_second[...] = jnp.where(zfirst, got, mine)
    l_pair[...] = mine + got
    l2_copy.start()

    def exp_row(ref, h):
        return jnp.exp(ref[pl.ds(h, 1), :])

    def combine_pair(h):
        up1(h).wait_recv()
        rate = wide(exp_row(l_second, h))
        one = jnp.ones_like(rate)
        rate_mine = jnp.where(zfirst, rate, one)
        rate_got = jnp.where(zfirst, one, rate)

        def total(quarter):
            at = pl.multiple_of(quarter * 64, 64)
            a = abuf[h, pl.ds(pl.multiple_of(u * 128 + at, 64), 64), :].astype(F32)
            b = r1[h, pl.ds(at, 64), :].astype(F32)
            return rate_mine * a + rate_got * b

        b2s[h] = total(1 - w).astype(BF16)
        up2(h).start()
        bk[h] = total(w)

    def share_rates():
        l2_copy.wait_recv()
        own_pair, got_pair = l_pair[...], l_z2[...]
        l_p0[...] = jnp.where(w == 0, own_pair, got_pair)
        l_p1[...] = jnp.where(w == 0, got_pair, own_pair)
        total = own_pair + got_pair
        l_line[...] = total
        l_x[LINES - 1] = total
        for k in range(1, LINES):
            remote(
                l_line,
                l_x.at[LINES - 1 - k],
                lsem.at[4],
                lsem.at[5],
                line_device(lax.rem(m + k, LINES)),
            ).start()

    rates_wait = remote(
        l_x.at[pl.ds(0, LINES - 1)], l_x.at[pl.ds(0, LINES - 1)], lsem.at[4], lsem.at[5], zp1
    )

    def combine_line(h):
        up2(h).wait_recv()
        rate = wide(exp_row(l_p1, h))
        one = jnp.ones_like(rate)
        total = jnp.where(w == 0, rate, one) * bk[h] + jnp.where(w == 0, one, rate) * r2[h].astype(F32)
        low = total.astype(BF16)
        for line in range(LINES):
            r, s = 16 * (line // 4), 128 * (line % 4)
            bt[h, line] = low[r : r + 16, s : s + 128]
        for k in range(1, LINES):
            x_send(h, k).start()
        r3[h, LINES - 1] = bt[h, m]

    def scan_lines(h):
        all_lines(r3, 0, h).wait_recv()
        carry = jnp.zeros((16, 128), F32)
        for line in range(LINES):
            slot = slot_of(line)
            low = carry.astype(BF16)
            tt[h, slot] = low
            if line < LINES - 1:
                rate = jnp.exp(l_x[slot, pl.ds(h, 1), :])
                carry = rate * carry + r3[h, slot].astype(F32)
        for k in range(1, LINES):
            y_send(h, k).start()
        tb[h, LINES - 1] = tt[h, LINES - 1]

    def carry_pairs(h):
        all_lines(tb, 1, h).wait_recv()
        rate = exp_row(l_p0, h)
        base = w * 64
        for line in range(LINES):
            r, s = 16 * (line // 4), 128 * (line % 4)
            start = tb[h, slot_of(line)].astype(F32)
            first_pair = jnp.where(
                w == 0, bk[h, r : r + 16, s : s + 128], r2[h, r : r + 16, s : s + 128].astype(F32)
            )
            after = rate * start + first_pair
            rows = pl.ds(pl.multiple_of(base + r, 16), 16)
            c2s[h, r : r + 16, s : s + 128] = jnp.where(w == 0, after, start).astype(BF16)
            cb[h, rows, s : s + 128] = jnp.where(w == 0, start, after).astype(BF16)
        down2(h, w).start()

    def carry_chips(h):
        down2(h, 1 - w).wait_recv()
        rate = wide(exp_row(l_first, h))
        for r in (0, 64):
            start = cb[h, r : r + 64, :].astype(F32)
            own_rows = pl.ds(pl.multiple_of(u * 128 + r, 64), 64)
            addition = jnp.where(zfirst, abuf[h, own_rows, :], r1[h, r : r + 64, :])
            after = rate * start + addition.astype(F32)
            s1s[h, r : r + 64, :] = jnp.where(zfirst, after, start).astype(BF16)
            sb[h, own_rows, :] = jnp.where(zfirst, start, after).astype(BF16)
        down1(h, half_mine).start()

    def within_block(h):
        @pl.when(h == 0)
        def _():
            all_arrived(2)

        for tile in range(2):
            keys = ROWS * (tile + 1)
            rows = slice(ROWS * tile, ROWS * (tile + 1))
            scores = lax.dot_general(
                qs[h, rows, :],
                ks[h, :keys, :],
                (((1,), (1,)), ((), ())),
                preferred_element_type=F32,
            )
            left = runb[h, rows, :]
            spread = jnp.concatenate([left] * (keys // 128), axis=1) - runt[pl.ds(h, 1), :keys]
            i = lax.broadcasted_iota(jnp.int32, (ROWS, keys), 0) + ROWS * tile
            j = lax.broadcasted_iota(jnp.int32, (ROWS, keys), 1)
            factor = jnp.exp(jnp.where(i >= j, spread, -jnp.inf))
            weights = (scores * factor).astype(BF16)
            within[h, rows, :] = jnp.dot(weights, vs[h, :keys, :], preferred_element_type=F32)

    def out_cross(h, core):
        return remote(
            obuf.at[h], o_ref.at[:, columns(core, h, DV)], osem.at[0], osem.at[1], partner
        )

    def finish(h):
        @pl.when(h == 0)
        def _():
            all_arrived(3)

        down1(h, half_other).wait_recv()
        state = sb[h]

        def gated_rows(first, tile):
            rows = pl.ds(pl.multiple_of(first * ROWS + 128 * tile, 128), 128)
            across = jnp.dot(qs[h, rows, :], state, preferred_element_type=F32)
            retained = within[h, rows, :] + across * wide(erunb[h, rows, :])
            retained = retained.astype(BF16).astype(F32)
            centered = retained - jnp.mean(retained, axis=1, keepdims=True)
            variance = jnp.mean(centered * centered, axis=1, keepdims=True)
            normed = centered * lax.rsqrt(variance + 1e-6)
            gate = gs[h, rows, :].astype(F32)
            return (gate / (1.0 + jnp.exp(-gate)) * normed).astype(BF16)

        for tile in range(2):
            obuf[h, 128 * tile : 128 * (tile + 1), :] = gated_rows(1 - c, tile)
        out_cross(h, c).start()
        for tile in range(2):
            o_ref[128 * tile : 128 * (tile + 1), columns(c, h, DV)] = gated_rows(c, tile)

    @pl.loop(0, NH + 8)
    def _(t):
        def stage(lag, f):
            @pl.when((t >= lag) & (t < lag + NH))
            def _():
                f(t - lag)

        stage(0, combine_pair)

        @pl.when(t == 0)
        def _():
            share_rates()

        stage(6, carry_chips)

        @pl.when(t == 3)
        def _():
            rates_wait.wait_recv()

        stage(3, scan_lines)
        stage(8, finish)
        stage(1, combine_line)
        stage(4, carry_pairs)
        stage(0, within_block)

    d_cross.wait_send()
    l1_copy.wait_send()
    l2_copy.wait_send()
    rates_wait.wait_send()

    def all_sent(ref, sem):
        remote(ref, ref, sem, osem.at[1], partner).wait_send()

    for n in range(4):
        all_sent(big[n][1].at[:, my_rows], d2s.at[n])
    all_sent(r1, ups.at[0])
    all_sent(r2, ups.at[1])
    all_sent(c2s, ups.at[2])
    all_sent(s1s, ups.at[3])
    all_sent(r3.at[:, pl.ds(0, LINES - 1)], xs.at[0])
    all_sent(tb.at[:, pl.ds(0, LINES - 1)], xs.at[1])
    all_sent(obuf, osem.at[0])
    others = o_ref.at[:, pl.ds(pl.multiple_of((1 - c) * NH * DV, NH * DV), NH * DV)]
    remote(others, others, osem.at[0], osem.at[1], partner).wait_recv()


def shards(queries, key_vectors, values, decay_log, gate_input):
    anywhere = pl.BlockSpec(memory_space=pl.ANY)
    tile = pltpu.VMEM((NH, 128), F32)
    dma = pltpu.SemaphoreType.DMA
    return pl.pallas_call(
        body,
        out_shape=pltpu.VMEM((ROWS, HEADS * DV), BF16),
        in_specs=[anywhere] * 5,
        out_specs=pl.BlockSpec(memory_space=pltpu.VMEM),
        scratch_shapes=[
            pltpu.VMEM((NH, BLOCK, DK), BF16),
            pltpu.VMEM((NH, BLOCK, DK), BF16),
            pltpu.VMEM((NH, BLOCK, DV), BF16),
            pltpu.VMEM((NH, BLOCK, DV), BF16),
            pltpu.VMEM((HEADS, BLOCK), BF16),
            pltpu.VMEM((NH, BLOCK, 128), F32),
            pltpu.VMEM((NH, BLOCK, 128), F32),
            pltpu.VMEM((NH, BLOCK, 128), F32),
            pltpu.VMEM((NH, BLOCK), F32),
            pltpu.VMEM((NH, DK, DV), BF16),
            pltpu.VMEM((NH, 128, DV), BF16),
            pltpu.VMEM((NH, 64, DV), F32),
            pltpu.VMEM((NH, 64, DV), BF16),
            pltpu.VMEM((NH, 64, DV), BF16),
            pltpu.VMEM((NH, LINES, 16, 128), BF16),
            pltpu.VMEM((NH, LINES, 16, 128), BF16),
            pltpu.VMEM((NH, LINES, 16, 128), BF16),
            pltpu.VMEM((NH, LINES, 16, 128), BF16),
            pltpu.VMEM((NH, 64, DV), BF16),
            pltpu.VMEM((NH, 128, DV), BF16),
            pltpu.VMEM((NH, 128, DV), BF16),
            pltpu.VMEM((NH, DK, DV), BF16),
            pltpu.VMEM((NH, BLOCK, DV), F32),
            pltpu.VMEM((NH, ROWS, DV), BF16),
            *[tile] * 9,
            pltpu.VMEM((LINES, NH, 128), F32),
            dma((4, NH)),
            dma((4,)),
            dma((4, NH)),
            dma((3,)),
            dma((6,)),
            dma((4,)),
            dma((4, NH)),
            dma((2,)),
            dma((2, NH)),
            dma((2,)),
        ],
        compiler_params=pltpu.CompilerParams(
            collective_id=0, has_side_effects=True, vmem_limit_bytes=VMEM
        ),
        name="retention",
    )(queries, key_vectors, values, decay_log.T, gate_input)


def solution(mesh):
    spec = P(("seq", "head"), None)
    return jax.shard_map(
        shards, mesh=mesh, in_specs=(spec,) * 5, out_specs=spec, check_vma=False
    )
```

```python
import jax
import jax.numpy as jnp
from jax import lax
from jax.experimental import pallas as pl
from jax.experimental.pallas import tpu as pltpu
from jax.sharding import PartitionSpec as P

MESH = pl.DeviceIdType.MESH
HEADS = 16
NH = 8
DK = 256
DV = 512
BLOCK = 512
ROWS = 256
LINES = 16
F32 = jnp.float32
BF16 = jnp.bfloat16
VMEM = 52 * 1024 * 1024


def remote(src, dst, send_sem, recv_sem, device):
    return pltpu.make_async_remote_copy(
        src_ref=src,
        dst_ref=dst,
        send_sem=send_sem,
        recv_sem=recv_sem,
        device_id=device,
        device_id_type=MESH,
    )


def wide(row):
    return jnp.concatenate([row] * (DV // 128), axis=1)


def body(
    q_hbm, k_hbm, v_hbm, d_hbm, g_hbm, o_ref,
    qs, ks, vs, gs, dl,
    runb, erunb, runt,
    abuf, r1, bk, b2s, r2, bt, r3, tt, tb, c2s, cb, s1s, sb, within, obuf,
    l_own, l_z1, l_first, l_second, l_pair, l_z2, l_p0, l_p1, l_line, l_x,
    loc, d2s, d2r, dsem, lsem, ups, upr, xs, xr, osem,
):
    x = lax.axis_index("seq")
    hd = lax.axis_index("head")
    c = lax.rem(hd, 2)
    zy = lax.div(hd, 2)
    z = lax.rem(zy, 4)
    y = lax.div(zy, 4)
    zfirst = lax.rem(z, 2) == 0
    u = lax.rem(lax.div(z + 1, 2), 2)
    w = lax.div(z, 2)
    m = x * 4 + y
    partner = (x, hd + 1 - 2 * c)
    zp1 = (x, (y * 4 + z + 1 - 2 * lax.rem(z, 2)) * 2 + c)
    zp2 = (x, (y * 4 + 3 - z) * 2 + c)

    def line_device(line):
        return (lax.div(line, 4), (lax.rem(line, 4) * 4 + z) * 2 + c)

    def slot_of(line):
        return lax.rem(line - m + 2 * LINES - 1, LINES)

    my_rows = pl.ds(pl.multiple_of(c * ROWS, ROWS), ROWS)
    other_rows = pl.ds(pl.multiple_of((1 - c) * ROWS, ROWS), ROWS)
    half_mine = pl.ds(pl.multiple_of(u * 128, 128), 128)
    half_other = pl.ds(pl.multiple_of((1 - u) * 128, 128), 128)

    big = ((k_hbm, ks, DK), (v_hbm, vs, DV), (q_hbm, qs, DK), (g_hbm, gs, DV))

    def columns(core, h, width):
        return pl.ds(pl.multiple_of((core * NH + h) * width, width), width)

    def arrival(sems, n, h):
        return sems.at[n, h] if n < 2 else sems.at[n, 0]

    def local_in(n, h):
        src, dst, width = big[n]
        return pltpu.make_async_copy(
            src.at[:, columns(c, h, width)], dst.at[h, my_rows], arrival(loc, n, h)
        )

    def cross_in(n, h):
        src, dst, width = big[n]
        return remote(
            src.at[:, columns(1 - c, h, width)],
            dst.at[h, my_rows],
            d2s.at[n],
            arrival(d2r, n, h),
            partner,
        )

    def cross_arrived(n, h):
        dst = big[n][1].at[h, other_rows]
        remote(dst, dst, d2s.at[n], arrival(d2r, n, h), partner).wait_recv()

    def all_arrived(n):
        own, got = big[n][1].at[:, my_rows], big[n][1].at[:, other_rows]
        pltpu.make_async_copy(own, own, loc.at[n, 0]).wait()
        remote(got, got, d2s.at[n], d2r.at[n, 0], partner).wait_recv()

    d_local = pltpu.make_async_copy(d_hbm, dl.at[:, my_rows], dsem.at[0])
    d_cross = remote(d_hbm, dl.at[:, my_rows], dsem.at[1], dsem.at[2], partner)

    barrier = pltpu.get_barrier_semaphore()
    peers = [partner, zp1, zp2] + [line_device(lax.rem(m + k, LINES)) for k in range(1, LINES)]
    for peer in peers:
        pl.semaphore_signal(barrier, inc=1, device_id=peer, device_id_type=MESH)

    d_local.start()

    @pl.loop(0, NH)
    def _(h):
        for n in range(2):
            local_in(n, h).start()

    pl.semaphore_wait(barrier, len(peers))

    d_cross.start()

    @pl.loop(0, NH)
    def _(h):
        cross_in(0, h).start()
        cross_in(1, h).start()

    row = lax.broadcasted_iota(jnp.int32, (BLOCK, BLOCK), 0)
    col = lax.broadcasted_iota(jnp.int32, (BLOCK, BLOCK), 1)
    lower = jnp.where(row >= col, 1.0, 0.0).astype(BF16)
    upper = jnp.where(row <= col, 1.0, 0.0).astype(BF16)
    d_local.wait()
    remote(d_hbm, dl.at[:, other_rows], dsem.at[1], dsem.at[2], partner).wait_recv()
    decays = dl[...]
    runt16 = jnp.dot(decays, upper, preferred_element_type=F32)
    run16 = lax.dot_general(
        lower, decays, (((1,), (1,)), ((), ())), preferred_element_type=F32
    )
    runt8 = jnp.where(c == 0, runt16[:NH], runt16[NH:])
    l_own[...] = jnp.broadcast_to(runt8[:, BLOCK - 1 : BLOCK], (NH, 128))
    runt[...] = runt8
    run8 = jnp.where(c == 0, run16[:, :NH], run16[:, NH:])
    fade8 = jnp.exp(run8[BLOCK - 1 : BLOCK] - run8)

    l1_copy = remote(l_own, l_z1, lsem.at[0], lsem.at[1], zp1)
    l2_copy = remote(l_pair, l_z2, lsem.at[2], lsem.at[3], zp2)

    def up1(h):
        return remote(abuf.at[h, half_other], r1.at[h], ups.at[0], upr.at[0, h], zp1)

    def up2(h):
        return remote(b2s.at[h], r2.at[h], ups.at[1], upr.at[1, h], zp2)

    def down2(h, quarter):
        rows = pl.ds(pl.multiple_of(quarter * 64, 64), 64)
        return remote(c2s.at[h], cb.at[h, rows], ups.at[2], upr.at[2, h], zp2)

    def down1(h, rows):
        return remote(s1s.at[h], sb.at[h, rows], ups.at[3], upr.at[3, h], zp1)

    def x_send(h, k):
        line = lax.rem(m + k, LINES)
        return remote(
            bt.at[h, line],
            r3.at[h, LINES - 1 - k],
            xs.at[0],
            xr.at[0, h],
            line_device(line),
        )

    def y_send(h, k):
        line = lax.rem(m + k, LINES)
        return remote(
            tt.at[h, k - 1],
            tb.at[h, LINES - 1 - k],
            xs.at[1],
            xr.at[1, h],
            line_device(line),
        )

    def all_lines(buffer, n, h):
        some = buffer.at[h, pl.ds(0, LINES - 1)]
        return remote(some, some, xs.at[n], xr.at[n, h], zp1)

    l1_copy.start()
    for h in range(NH):
        for n in range(2):
            local_in(n, h).wait()
            cross_arrived(n, h)
        fade = jnp.broadcast_to(fade8[:, h : h + 1], (BLOCK, DK))
        faded = (ks[h].astype(F32) * fade).astype(BF16)
        addition = lax.dot_general(
            faded, vs[h], (((0,), (0,)), ((), ())), preferred_element_type=F32
        )
        abuf[h] = addition.astype(BF16)
        up1(h).start()

    @pl.loop(0, NH)
    def _(h):
        local_in(2, h).start()
        cross_in(2, h).start()

    @pl.loop(0, NH)
    def _(h):
        local_in(3, h).start()
        cross_in(3, h).start()

    l1_copy.wait_recv()
    mine, got = l_own[...], l_z1[...]
    l_first[...] = jnp.where(zfirst, mine, got)
    l_second[...] = jnp.where(zfirst, got, mine)
    l_pair[...] = mine + got
    l2_copy.start()

    erun8 = jnp.exp(run8)
    for h in range(NH):
        runb[h] = jnp.broadcast_to(run8[:, h : h + 1], (BLOCK, 128))
        erunb[h] = jnp.broadcast_to(erun8[:, h : h + 1], (BLOCK, 128))

    def exp_row(ref, h):
        return jnp.exp(ref[pl.ds(h, 1), :])

    def combine_pair(h):
        up1(h).wait_recv()
        rate = wide(exp_row(l_second, h))
        one = jnp.ones_like(rate)
        rate_mine = jnp.where(zfirst, rate, one)
        rate_got = jnp.where(zfirst, one, rate)

        def total(quarter):
            at = pl.multiple_of(quarter * 64, 64)
            a = abuf[h, pl.ds(pl.multiple_of(u * 128 + at, 64), 64), :].astype(F32)
            b = r1[h, pl.ds(at, 64), :].astype(F32)
            return rate_mine * a + rate_got * b

        b2s[h] = total(1 - w).astype(BF16)
        up2(h).start()
        bk[h] = total(w)

    def share_rates():
        l2_copy.wait_recv()
        own_pair, got_pair = l_pair[...], l_z2[...]
        l_p0[...] = jnp.where(w == 0, own_pair, got_pair)
        l_p1[...] = jnp.where(w == 0, got_pair, own_pair)
        total = own_pair + got_pair
        l_line[...] = total
        l_x[LINES - 1] = total
        for k in range(1, LINES):
            remote(
                l_line,
                l_x.at[LINES - 1 - k],
                lsem.at[4],
                lsem.at[5],
                line_device(lax.rem(m + k, LINES)),
            ).start()

    rates_wait = remote(
        l_x.at[pl.ds(0, LINES - 1)], l_x.at[pl.ds(0, LINES - 1)], lsem.at[4], lsem.at[5], zp1
    )

    def combine_line(h):
        up2(h).wait_recv()
        rate = wide(exp_row(l_p1, h))
        one = jnp.ones_like(rate)
        total = jnp.where(w == 0, rate, one) * bk[h] + jnp.where(w == 0, one, rate) * r2[h].astype(F32)
        low = total.astype(BF16)
        for line in range(LINES):
            r, s = 16 * (line // 4), 128 * (line % 4)
            bt[h, line] = low[r : r + 16, s : s + 128]
        for k in range(1, LINES):
            x_send(h, k).start()
        r3[h, LINES - 1] = bt[h, m]

    def scan_lines(h):
        all_lines(r3, 0, h).wait_recv()
        carry = jnp.zeros((16, 128), F32)
        for line in range(LINES):
            slot = slot_of(line)
            low = carry.astype(BF16)
            tt[h, slot] = low
            if line < LINES - 1:
                rate = jnp.exp(l_x[slot, pl.ds(h, 1), :])
                carry = rate * carry + r3[h, slot].astype(F32)
        for k in range(1, LINES):
            y_send(h, k).start()
        tb[h, LINES - 1] = tt[h, LINES - 1]

    def carry_pairs(h):
        all_lines(tb, 1, h).wait_recv()
        rate = exp_row(l_p0, h)
        base = w * 64
        for line in range(LINES):
            r, s = 16 * (line // 4), 128 * (line % 4)
            start = tb[h, slot_of(line)].astype(F32)
            first_pair = jnp.where(
                w == 0, bk[h, r : r + 16, s : s + 128], r2[h, r : r + 16, s : s + 128].astype(F32)
            )
            after = rate * start + first_pair
            rows = pl.ds(pl.multiple_of(base + r, 16), 16)
            c2s[h, r : r + 16, s : s + 128] = jnp.where(w == 0, after, start).astype(BF16)
            cb[h, rows, s : s + 128] = jnp.where(w == 0, start, after).astype(BF16)
        down2(h, w).start()

    def carry_chips(h):
        down2(h, 1 - w).wait_recv()
        rate = wide(exp_row(l_first, h))
        for r in (0, 64):
            start = cb[h, r : r + 64, :].astype(F32)
            own_rows = pl.ds(pl.multiple_of(u * 128 + r, 64), 64)
            addition = jnp.where(zfirst, abuf[h, own_rows, :], r1[h, r : r + 64, :])
            after = rate * start + addition.astype(F32)
            s1s[h, r : r + 64, :] = jnp.where(zfirst, after, start).astype(BF16)
            sb[h, own_rows, :] = jnp.where(zfirst, start, after).astype(BF16)
        down1(h, half_mine).start()

    def within_block(h):
        @pl.when(h == 0)
        def _():
            all_arrived(2)

        for tile in range(2):
            keys = ROWS * (tile + 1)
            rows = slice(ROWS * tile, ROWS * (tile + 1))
            scores = lax.dot_general(
                qs[h, rows, :],
                ks[h, :keys, :],
                (((1,), (1,)), ((), ())),
                preferred_element_type=F32,
            )
            left = runb[h, rows, :]
            spread = jnp.concatenate([left] * (keys // 128), axis=1) - runt[pl.ds(h, 1), :keys]
            i = lax.broadcasted_iota(jnp.int32, (ROWS, keys), 0) + ROWS * tile
            j = lax.broadcasted_iota(jnp.int32, (ROWS, keys), 1)
            factor = jnp.exp(jnp.where(i >= j, spread, -jnp.inf))
            weights = (scores * factor).astype(BF16)
            within[h, rows, :] = jnp.dot(weights, vs[h, :keys, :], preferred_element_type=F32)

    def out_cross(h, core):
        return remote(
            obuf.at[h], o_ref.at[:, columns(core, h, DV)], osem.at[0], osem.at[1], partner
        )

    def finish(h):
        @pl.when(h == 0)
        def _():
            all_arrived(3)

        down1(h, half_other).wait_recv()
        state = sb[h]

        def gated_rows(first, tile):
            rows = pl.ds(pl.multiple_of(first * ROWS + 128 * tile, 128), 128)
            across = jnp.dot(qs[h, rows, :], state, preferred_element_type=F32)
            retained = within[h, rows, :] + across * wide(erunb[h, rows, :])
            retained = retained.astype(BF16).astype(F32)
            centered = retained - jnp.mean(retained, axis=1, keepdims=True)
            variance = jnp.mean(centered * centered, axis=1, keepdims=True)
            normed = centered * lax.rsqrt(variance + 1e-6)
            gate = gs[h, rows, :].astype(F32)
            return (gate / (1.0 + jnp.exp(-gate)) * normed).astype(BF16)

        for tile in range(2):
            obuf[h, 128 * tile : 128 * (tile + 1), :] = gated_rows(1 - c, tile)
        out_cross(h, c).start()
        for tile in range(2):
            o_ref[128 * tile : 128 * (tile + 1), columns(c, h, DV)] = gated_rows(c, tile)

    @pl.loop(0, NH + 8)
    def _(t):
        def stage(lag, f):
            @pl.when((t >= lag) & (t < lag + NH))
            def _():
                f(t - lag)

        stage(0, combine_pair)

        @pl.when(t == 0)
        def _():
            share_rates()

        stage(6, carry_chips)

        @pl.when(t == 3)
        def _():
            rates_wait.wait_recv()

        stage(3, scan_lines)
        stage(8, finish)
        stage(1, combine_line)
        stage(4, carry_pairs)
        stage(3, within_block)

    d_cross.wait_send()
    l1_copy.wait_send()
    l2_copy.wait_send()
    rates_wait.wait_send()

    def all_sent(ref, sem):
        remote(ref, ref, sem, osem.at[1], partner).wait_send()

    for n in range(4):
        all_sent(big[n][1].at[:, my_rows], d2s.at[n])
    all_sent(r1, ups.at[0])
    all_sent(r2, ups.at[1])
    all_sent(c2s, ups.at[2])
    all_sent(s1s, ups.at[3])
    all_sent(r3.at[:, pl.ds(0, LINES - 1)], xs.at[0])
    all_sent(tb.at[:, pl.ds(0, LINES - 1)], xs.at[1])
    all_sent(obuf, osem.at[0])
    others = o_ref.at[:, pl.ds(pl.multiple_of((1 - c) * NH * DV, NH * DV), NH * DV)]
    remote(others, others, osem.at[0], osem.at[1], partner).wait_recv()


def shards(queries, key_vectors, values, decay_log, gate_input):
    anywhere = pl.BlockSpec(memory_space=pl.ANY)
    tile = pltpu.VMEM((NH, 128), F32)
    dma = pltpu.SemaphoreType.DMA
    return pl.pallas_call(
        body,
        out_shape=pltpu.VMEM((ROWS, HEADS * DV), BF16),
        in_specs=[anywhere] * 5,
        out_specs=pl.BlockSpec(memory_space=pltpu.VMEM),
        scratch_shapes=[
            pltpu.VMEM((NH, BLOCK, DK), BF16),
            pltpu.VMEM((NH, BLOCK, DK), BF16),
            pltpu.VMEM((NH, BLOCK, DV), BF16),
            pltpu.VMEM((NH, BLOCK, DV), BF16),
            pltpu.VMEM((HEADS, BLOCK), BF16),
            pltpu.VMEM((NH, BLOCK, 128), F32),
            pltpu.VMEM((NH, BLOCK, 128), F32),
            pltpu.VMEM((NH, BLOCK), F32),
            pltpu.VMEM((NH, DK, DV), BF16),
            pltpu.VMEM((NH, 128, DV), BF16),
            pltpu.VMEM((NH, 64, DV), F32),
            pltpu.VMEM((NH, 64, DV), BF16),
            pltpu.VMEM((NH, 64, DV), BF16),
            pltpu.VMEM((NH, LINES, 16, 128), BF16),
            pltpu.VMEM((NH, LINES, 16, 128), BF16),
            pltpu.VMEM((NH, LINES, 16, 128), BF16),
            pltpu.VMEM((NH, LINES, 16, 128), BF16),
            pltpu.VMEM((NH, 64, DV), BF16),
            pltpu.VMEM((NH, 128, DV), BF16),
            pltpu.VMEM((NH, 128, DV), BF16),
            pltpu.VMEM((NH, DK, DV), BF16),
            pltpu.VMEM((NH, BLOCK, DV), F32),
            pltpu.VMEM((NH, ROWS, DV), BF16),
            *[tile] * 9,
            pltpu.VMEM((LINES, NH, 128), F32),
            dma((4, NH)),
            dma((4,)),
            dma((4, NH)),
            dma((3,)),
            dma((6,)),
            dma((4,)),
            dma((4, NH)),
            dma((2,)),
            dma((2, NH)),
            dma((2,)),
        ],
        compiler_params=pltpu.CompilerParams(
            collective_id=0, has_side_effects=True, vmem_limit_bytes=VMEM
        ),
        name="retention",
    )(queries, key_vectors, values, decay_log.T, gate_input)


def solution(mesh):
    spec = P(("seq", "head"), None)
    return jax.shard_map(
        shards, mesh=mesh, in_specs=(spec,) * 5, out_specs=spec, check_vma=False
    )
```

```python
import jax
import jax.numpy as jnp
from jax import lax
from jax.experimental import pallas as pl
from jax.experimental.pallas import tpu as pltpu
from jax.sharding import PartitionSpec as P

MESH = pl.DeviceIdType.MESH
HEADS = 16
NH = 8
DK = 256
DV = 512
BLOCK = 512
ROWS = 256
LINES = 16
F32 = jnp.float32
BF16 = jnp.bfloat16
VMEM = 52 * 1024 * 1024


def remote(src, dst, send_sem, recv_sem, device):
    return pltpu.make_async_remote_copy(
        src_ref=src,
        dst_ref=dst,
        send_sem=send_sem,
        recv_sem=recv_sem,
        device_id=device,
        device_id_type=MESH,
    )


def wide(row):
    return jnp.concatenate([row] * (DV // 128), axis=1)


def body(
    q_hbm, k_hbm, v_hbm, d_hbm, g_hbm, o_ref,
    qs, ks, vs, gs, dl,
    runb, erunb, runt,
    abuf, r1, bk, b2s, r2, bt, r3, tt, tb, c2s, cb, s1s, sb, within, obuf,
    l_own, l_z1, l_first, l_second, l_pair, l_z2, l_p0, l_p1, l_line, l_x,
    loc, d2s, d2r, dsem, lsem, ups, upr, xs, xr, osem,
):
    x = lax.axis_index("seq")
    hd = lax.axis_index("head")
    c = lax.rem(hd, 2)
    zy = lax.div(hd, 2)
    z = lax.rem(zy, 4)
    y = lax.div(zy, 4)
    zfirst = lax.rem(z, 2) == 0
    u = lax.rem(lax.div(z + 1, 2), 2)
    w = lax.div(z, 2)
    m = x * 4 + y
    partner = (x, hd + 1 - 2 * c)
    zp1 = (x, (y * 4 + z + 1 - 2 * lax.rem(z, 2)) * 2 + c)
    zp2 = (x, (y * 4 + 3 - z) * 2 + c)

    def line_device(line):
        return (lax.div(line, 4), (lax.rem(line, 4) * 4 + z) * 2 + c)

    def slot_of(line):
        return lax.rem(line - m + 2 * LINES - 1, LINES)

    my_rows = pl.ds(pl.multiple_of(c * ROWS, ROWS), ROWS)
    other_rows = pl.ds(pl.multiple_of((1 - c) * ROWS, ROWS), ROWS)
    half_mine = pl.ds(pl.multiple_of(u * 128, 128), 128)
    half_other = pl.ds(pl.multiple_of((1 - u) * 128, 128), 128)

    big = ((k_hbm, ks, DK), (v_hbm, vs, DV), (q_hbm, qs, DK), (g_hbm, gs, DV))

    def columns(core, h, width):
        return pl.ds(pl.multiple_of((core * NH + h) * width, width), width)

    def arrival(sems, n, h):
        return sems.at[n, h] if n < 2 else sems.at[n, 0]

    def local_in(n, h):
        src, dst, width = big[n]
        return pltpu.make_async_copy(
            src.at[:, columns(c, h, width)], dst.at[h, my_rows], arrival(loc, n, h)
        )

    def cross_in(n, h):
        src, dst, width = big[n]
        return remote(
            src.at[:, columns(1 - c, h, width)],
            dst.at[h, my_rows],
            d2s.at[n],
            arrival(d2r, n, h),
            partner,
        )

    def cross_arrived(n, h):
        dst = big[n][1].at[h, other_rows]
        remote(dst, dst, d2s.at[n], arrival(d2r, n, h), partner).wait_recv()

    def all_arrived(n):
        own, got = big[n][1].at[:, my_rows], big[n][1].at[:, other_rows]
        pltpu.make_async_copy(own, own, loc.at[n, 0]).wait()
        remote(got, got, d2s.at[n], d2r.at[n, 0], partner).wait_recv()

    d_local = pltpu.make_async_copy(d_hbm, dl.at[:, my_rows], dsem.at[0])
    d_cross = remote(d_hbm, dl.at[:, my_rows], dsem.at[1], dsem.at[2], partner)

    barrier = pltpu.get_barrier_semaphore()
    peers = [partner, zp1, zp2] + [line_device(lax.rem(m + k, LINES)) for k in range(1, LINES)]
    for peer in peers:
        pl.semaphore_signal(barrier, inc=1, device_id=peer, device_id_type=MESH)

    d_local.start()

    @pl.loop(0, NH)
    def _(h):
        for n in range(2):
            local_in(n, h).start()

    pl.semaphore_wait(barrier, len(peers))

    d_cross.start()

    @pl.loop(0, NH)
    def _(h):
        cross_in(0, h).start()
        cross_in(1, h).start()

    row = lax.broadcasted_iota(jnp.int32, (BLOCK, BLOCK), 0)
    col = lax.broadcasted_iota(jnp.int32, (BLOCK, BLOCK), 1)
    lower = jnp.where(row >= col, 1.0, 0.0).astype(BF16)
    upper = jnp.where(row <= col, 1.0, 0.0).astype(BF16)
    d_local.wait()
    remote(d_hbm, dl.at[:, other_rows], dsem.at[1], dsem.at[2], partner).wait_recv()
    decays = dl[...]
    runt16 = jnp.dot(decays, upper, preferred_element_type=F32)
    run16 = lax.dot_general(
        lower, decays, (((1,), (1,)), ((), ())), preferred_element_type=F32
    )
    runt8 = jnp.where(c == 0, runt16[:NH], runt16[NH:])
    l_own[...] = jnp.broadcast_to(runt8[:, BLOCK - 1 : BLOCK], (NH, 128))
    runt[...] = runt8
    run8 = jnp.where(c == 0, run16[:, :NH], run16[:, NH:])
    fade8 = jnp.exp(run8[BLOCK - 1 : BLOCK] - run8)

    l1_copy = remote(l_own, l_z1, lsem.at[0], lsem.at[1], zp1)
    l2_copy = remote(l_pair, l_z2, lsem.at[2], lsem.at[3], zp2)

    def up1(h):
        return remote(abuf.at[h, half_other], r1.at[h], ups.at[0], upr.at[0, h], zp1)

    def up2(h):
        return remote(b2s.at[h], r2.at[h], ups.at[1], upr.at[1, h], zp2)

    def down2(h, quarter):
        rows = pl.ds(pl.multiple_of(quarter * 64, 64), 64)
        return remote(c2s.at[h], cb.at[h, rows], ups.at[2], upr.at[2, h], zp2)

    def down1(h, rows):
        return remote(s1s.at[h], sb.at[h, rows], ups.at[3], upr.at[3, h], zp1)

    def x_send(h, k):
        line = lax.rem(m + k, LINES)
        return remote(
            bt.at[h, line],
            r3.at[h, LINES - 1 - k],
            xs.at[0],
            xr.at[0, h],
            line_device(line),
        )

    def y_send(h, k):
        line = lax.rem(m + k, LINES)
        return remote(
            tt.at[h, k - 1],
            tb.at[h, LINES - 1 - k],
            xs.at[1],
            xr.at[1, h],
            line_device(line),
        )

    def all_lines(buffer, n, h):
        some = buffer.at[h, pl.ds(0, LINES - 1)]
        return remote(some, some, xs.at[n], xr.at[n, h], zp1)

    l1_copy.start()
    for h in range(NH):
        for n in range(2):
            local_in(n, h).wait()
            cross_arrived(n, h)
        fade = jnp.broadcast_to(fade8[:, h : h + 1], (BLOCK, DK))
        faded = (ks[h].astype(F32) * fade).astype(BF16)
        addition = lax.dot_general(
            faded, vs[h], (((0,), (0,)), ((), ())), preferred_element_type=F32
        )
        abuf[h] = addition.astype(BF16)
        up1(h).start()

    @pl.loop(0, NH)
    def _(h):
        local_in(2, h).start()
        cross_in(2, h).start()

    @pl.loop(0, NH)
    def _(h):
        local_in(3, h).start()
        cross_in(3, h).start()

    l1_copy.wait_recv()
    mine, got = l_own[...], l_z1[...]
    l_first[...] = jnp.where(zfirst, mine, got)
    l_second[...] = jnp.where(zfirst, got, mine)
    l_pair[...] = mine + got
    l2_copy.start()

    erun8 = jnp.exp(run8)
    for h in range(NH):
        runb[h] = jnp.broadcast_to(run8[:, h : h + 1], (BLOCK, 128))
        erunb[h] = jnp.broadcast_to(erun8[:, h : h + 1], (BLOCK, 128))

    def exp_row(ref, h):
        return jnp.exp(ref[pl.ds(h, 1), :])

    def combine_pair(h):
        up1(h).wait_recv()
        rate = wide(exp_row(l_second, h))
        one = jnp.ones_like(rate)
        rate_mine = jnp.where(zfirst, rate, one)
        rate_got = jnp.where(zfirst, one, rate)

        def total(quarter):
            at = pl.multiple_of(quarter * 64, 64)
            a = abuf[h, pl.ds(pl.multiple_of(u * 128 + at, 64), 64), :].astype(F32)
            b = r1[h, pl.ds(at, 64), :].astype(F32)
            return rate_mine * a + rate_got * b

        b2s[h] = total(1 - w).astype(BF16)
        up2(h).start()
        bk[h] = total(w)

    def share_rates():
        l2_copy.wait_recv()
        own_pair, got_pair = l_pair[...], l_z2[...]
        l_p0[...] = jnp.where(w == 0, own_pair, got_pair)
        l_p1[...] = jnp.where(w == 0, got_pair, own_pair)
        total = own_pair + got_pair
        l_line[...] = total
        l_x[LINES - 1] = total
        for k in range(1, LINES):
            remote(
                l_line,
                l_x.at[LINES - 1 - k],
                lsem.at[4],
                lsem.at[5],
                line_device(lax.rem(m + k, LINES)),
            ).start()

    rates_wait = remote(
        l_x.at[pl.ds(0, LINES - 1)], l_x.at[pl.ds(0, LINES - 1)], lsem.at[4], lsem.at[5], zp1
    )

    def combine_line(h):
        up2(h).wait_recv()
        rate = wide(exp_row(l_p1, h))
        one = jnp.ones_like(rate)
        total = jnp.where(w == 0, rate, one) * bk[h] + jnp.where(w == 0, one, rate) * r2[h].astype(F32)
        low = total.astype(BF16)
        for line in range(LINES):
            r, s = 16 * (line // 4), 128 * (line % 4)
            bt[h, line] = low[r : r + 16, s : s + 128]
        for k in range(1, LINES):
            x_send(h, k).start()
        r3[h, LINES - 1] = bt[h, m]

    def scan_lines(h):
        all_lines(r3, 0, h).wait_recv()
        carry = jnp.zeros((16, 128), F32)
        for line in range(LINES):
            slot = slot_of(line)
            low = carry.astype(BF16)
            tt[h, slot] = low
            if line < LINES - 1:
                rate = jnp.exp(l_x[slot, pl.ds(h, 1), :])
                carry = rate * carry + r3[h, slot].astype(F32)
        for k in range(1, LINES):
            y_send(h, k).start()
        tb[h, LINES - 1] = tt[h, LINES - 1]

    def carry_pairs(h):
        all_lines(tb, 1, h).wait_recv()
        rate = exp_row(l_p0, h)
        base = w * 64
        for line in range(LINES):
            r, s = 16 * (line // 4), 128 * (line % 4)
            start = tb[h, slot_of(line)].astype(F32)
            first_pair = jnp.where(
                w == 0, bk[h, r : r + 16, s : s + 128], r2[h, r : r + 16, s : s + 128].astype(F32)
            )
            after = rate * start + first_pair
            rows = pl.ds(pl.multiple_of(base + r, 16), 16)
            c2s[h, r : r + 16, s : s + 128] = jnp.where(w == 0, after, start).astype(BF16)
            cb[h, rows, s : s + 128] = jnp.where(w == 0, start, after).astype(BF16)
        down2(h, w).start()

    def carry_chips(h):
        down2(h, 1 - w).wait_recv()
        rate = wide(exp_row(l_first, h))
        for r in (0, 64):
            start = cb[h, r : r + 64, :].astype(F32)
            own_rows = pl.ds(pl.multiple_of(u * 128 + r, 64), 64)
            addition = jnp.where(zfirst, abuf[h, own_rows, :], r1[h, r : r + 64, :])
            after = rate * start + addition.astype(F32)
            s1s[h, r : r + 64, :] = jnp.where(zfirst, after, start).astype(BF16)
            sb[h, own_rows, :] = jnp.where(zfirst, start, after).astype(BF16)
        down1(h, half_mine).start()

    def within_block(h):
        @pl.when(h == 0)
        def _():
            all_arrived(2)

        for tile in range(2):
            keys = ROWS * (tile + 1)
            rows = slice(ROWS * tile, ROWS * (tile + 1))
            scores = lax.dot_general(
                qs[h, rows, :],
                ks[h, :keys, :],
                (((1,), (1,)), ((), ())),
                preferred_element_type=F32,
            )
            left = runb[h, rows, :]
            spread = jnp.concatenate([left] * (keys // 128), axis=1) - runt[pl.ds(h, 1), :keys]
            i = lax.broadcasted_iota(jnp.int32, (ROWS, keys), 0) + ROWS * tile
            j = lax.broadcasted_iota(jnp.int32, (ROWS, keys), 1)
            factor = jnp.exp(jnp.where(i >= j, spread, -jnp.inf))
            weights = (scores * factor).astype(BF16)
            within[h, rows, :] = jnp.dot(weights, vs[h, :keys, :], preferred_element_type=F32)

    def out_cross(h, core, tile):
        rows = pl.ds(128 * tile, 128)
        return remote(
            obuf.at[h, rows],
            o_ref.at[rows, columns(core, h, DV)],
            osem.at[0],
            osem.at[1],
            partner,
        )

    def finish(h):
        @pl.when(h == 0)
        def _():
            all_arrived(3)

        down1(h, half_other).wait_recv()
        state = sb[h]

        def gated_rows(first, tile):
            rows = pl.ds(pl.multiple_of(first * ROWS + 128 * tile, 128), 128)
            across = jnp.dot(qs[h, rows, :], state, preferred_element_type=F32)
            retained = within[h, rows, :] + across * wide(erunb[h, rows, :])
            retained = retained.astype(BF16).astype(F32)
            centered = retained - jnp.mean(retained, axis=1, keepdims=True)
            variance = jnp.mean(centered * centered, axis=1, keepdims=True)
            normed = centered * lax.rsqrt(variance + 1e-6)
            gate = gs[h, rows, :].astype(F32)
            return (gate / (1.0 + jnp.exp(-gate)) * normed).astype(BF16)

        for tile in range(2):
            obuf[h, 128 * tile : 128 * (tile + 1), :] = gated_rows(1 - c, tile)
            out_cross(h, c, tile).start()
        for tile in range(2):
            o_ref[128 * tile : 128 * (tile + 1), columns(c, h, DV)] = gated_rows(c, tile)

    @pl.loop(0, NH + 8)
    def _(t):
        def stage(lag, f):
            @pl.when((t >= lag) & (t < lag + NH))
            def _():
                f(t - lag)

        stage(0, combine_pair)

        @pl.when(t == 0)
        def _():
            share_rates()

        stage(6, carry_chips)

        @pl.when(t == 3)
        def _():
            rates_wait.wait_recv()

        stage(3, scan_lines)
        stage(8, finish)
        stage(1, combine_line)
        stage(4, carry_pairs)
        stage(3, within_block)

    d_cross.wait_send()
    l1_copy.wait_send()
    l2_copy.wait_send()
    rates_wait.wait_send()

    def all_sent(ref, sem):
        remote(ref, ref, sem, osem.at[1], partner).wait_send()

    for n in range(4):
        all_sent(big[n][1].at[:, my_rows], d2s.at[n])
    all_sent(r1, ups.at[0])
    all_sent(r2, ups.at[1])
    all_sent(c2s, ups.at[2])
    all_sent(s1s, ups.at[3])
    all_sent(r3.at[:, pl.ds(0, LINES - 1)], xs.at[0])
    all_sent(tb.at[:, pl.ds(0, LINES - 1)], xs.at[1])
    all_sent(obuf, osem.at[0])
    others = o_ref.at[:, pl.ds(pl.multiple_of((1 - c) * NH * DV, NH * DV), NH * DV)]
    remote(others, others, osem.at[0], osem.at[1], partner).wait_recv()


def shards(queries, key_vectors, values, decay_log, gate_input):
    anywhere = pl.BlockSpec(memory_space=pl.ANY)
    tile = pltpu.VMEM((NH, 128), F32)
    dma = pltpu.SemaphoreType.DMA
    return pl.pallas_call(
        body,
        out_shape=pltpu.VMEM((ROWS, HEADS * DV), BF16),
        in_specs=[anywhere] * 5,
        out_specs=pl.BlockSpec(memory_space=pltpu.VMEM),
        scratch_shapes=[
            pltpu.VMEM((NH, BLOCK, DK), BF16),
            pltpu.VMEM((NH, BLOCK, DK), BF16),
            pltpu.VMEM((NH, BLOCK, DV), BF16),
            pltpu.VMEM((NH, BLOCK, DV), BF16),
            pltpu.VMEM((HEADS, BLOCK), BF16),
            pltpu.VMEM((NH, BLOCK, 128), F32),
            pltpu.VMEM((NH, BLOCK, 128), F32),
            pltpu.VMEM((NH, BLOCK), F32),
            pltpu.VMEM((NH, DK, DV), BF16),
            pltpu.VMEM((NH, 128, DV), BF16),
            pltpu.VMEM((NH, 64, DV), F32),
            pltpu.VMEM((NH, 64, DV), BF16),
            pltpu.VMEM((NH, 64, DV), BF16),
            pltpu.VMEM((NH, LINES, 16, 128), BF16),
            pltpu.VMEM((NH, LINES, 16, 128), BF16),
            pltpu.VMEM((NH, LINES, 16, 128), BF16),
            pltpu.VMEM((NH, LINES, 16, 128), BF16),
            pltpu.VMEM((NH, 64, DV), BF16),
            pltpu.VMEM((NH, 128, DV), BF16),
            pltpu.VMEM((NH, 128, DV), BF16),
            pltpu.VMEM((NH, DK, DV), BF16),
            pltpu.VMEM((NH, BLOCK, DV), F32),
            pltpu.VMEM((NH, ROWS, DV), BF16),
            *[tile] * 9,
            pltpu.VMEM((LINES, NH, 128), F32),
            dma((4, NH)),
            dma((4,)),
            dma((4, NH)),
            dma((3,)),
            dma((6,)),
            dma((4,)),
            dma((4, NH)),
            dma((2,)),
            dma((2, NH)),
            dma((2,)),
        ],
        compiler_params=pltpu.CompilerParams(
            collective_id=0, has_side_effects=True, vmem_limit_bytes=VMEM
        ),
        name="retention",
    )(queries, key_vectors, values, decay_log.T, gate_input)


def solution(mesh):
    spec = P(("seq", "head"), None)
    return jax.shard_map(
        shards, mesh=mesh, in_specs=(spec,) * 5, out_specs=spec, check_vma=False
    )
```
